32 devices in a mesh: section: 2 (over y), mp: 16 (over z, x, core).
Axes of the slice: x: 2, y: 2, z: 4, core: 2. Of those that a mesh axis runs over, the one named last changes fastest.
Arguments:
- features: bfloat16 [4, 32, 8192], P(None, None, 'mp'), may hold values from -6 to 6
- labels: int32 [4, 32], replicated, may hold values 0 or 1
- weights: bfloat16 [2, 8192, 8192], P('section', None, 'mp'), may hold values from -1.78986404 to 1.78986404
- vectors: float32 [2, 8192], P('section', 'mp'), may hold values from -6 to 6
- head_weight: float32 [8192], P('mp'), may hold values from -0.0625 to 0.0625
Outputs:
- weight_grad: bfloat16 [2, 8192, 8192], P('section', None, 'mp')
- new_vectors: float32 [2, 8192], P('section', 'mp')
- rank_coef: float32 [2], P('section')
The draws below stay inside these ranges and needn't reach their ends.
All inputs are finite; a program needn't handle non-finite values.
Results may differ from the reference program's by a relative error of at most 0.015.
Values may be sent and summed in bfloat16 or wider, within the bound.
No kernel may reach another device: no remote copies, remote signals or barrier semaphores. Data moves between devices by JAX's collectives and lax.ppermute only.
A program may use at most 64 MiB of HBM per device.

```python
import math
import jax
import jax.numpy as jnp
from jax import lax

D = 8192
MICRO = 4
BATCH = 32
LAYERS = 2


def draw_weights(key, part):
    key_base = jax.random.fold_in(key, 11)
    key_list = jax.random.split(key_base, 3)
    base_draw = jnp.clip(jax.random.normal(key_list[0], (LAYERS, D, D), jnp.float32), -6.0, 6.0)
    low_scale = 0.5
    high_scale = 2.0
    row_scale = jnp.exp(jax.random.uniform(key_list[1], (LAYERS, D, 1), jnp.float32, math.log(low_scale), math.log(high_scale)))
    col_scale = jnp.exp(jax.random.uniform(key_list[2], (LAYERS, 1, D), jnp.float32, math.log(low_scale), math.log(high_scale)))
    col_ramp = jnp.exp(math.log(3.0) * jnp.arange(D, dtype=jnp.float32) / D)
    scaled = base_draw * row_scale * col_scale * col_ramp[None, None, :] / math.sqrt(D)
    return scaled.astype(jnp.bfloat16)


def with_ends(values, key, smallest, largest):
    longest = values.shape.index(max(values.shape))
    spots = []
    for shift in (0, 1):
        where = [jax.random.randint(jax.random.fold_in(key, axis), (), 0, length) for axis, length in enumerate(values.shape)]
        where[longest] = (where[longest] + shift) % values.shape[longest]
        spots.append(tuple(where))
    return values.at[spots[0]].set(smallest).at[spots[1]].set(largest)


def levels(stream_key, dims, shards, smallest, top_value):
    def one(position, shards_of):
        steps = jax.random.uniform(jax.random.fold_in(jax.random.fold_in(stream_key, 6), position), (shards_of,), jnp.float32, smallest / len(shards), top_value / len(shards))
        return jnp.repeat(jnp.exp(steps), dims[position] // shards_of).reshape((-1,) + (1,) * (len(dims) - position - 1))

    factor_of = one(*shards[0])
    for cut in shards[1:]:
        factor_of = factor_of * one(*cut)
    return factor_of


def normal_values(own_key, dims, spread, reach, shards=(), kind=jnp.bfloat16):
    array = spread * jax.random.normal(own_key, dims, jnp.float32)
    if shards:
        array = array * levels(own_key, dims, shards, -0.22, 0.18)
    return jnp.clip(array, -reach, reach).astype(kind)


def setup_inputs(seed: int = 0) -> dict:
    seeds = jax.random.split(jax.random.key(seed), 6)
    features = normal_values(seeds[0], (MICRO, BATCH, D), 1.0, 6.0, ((2, 16),))
    labels = with_ends((jax.random.randint(seeds[1], (MICRO, BATCH), 0, 2) < 1).astype(jnp.int32), jax.random.fold_in(seeds[1], 1), 0, 1)
    weights = draw_weights(jax.random.fold_in(seeds[5], 71), 0)
    vectors = normal_values(seeds[3], (LAYERS, D), 1.0, 6.0, ((0, 2), (1, 16)), jnp.float32)
    head_weight = normal_values(seeds[4], (D,), D ** -0.5, 0.0625, ((0, 16),), jnp.float32)
    return dict(features=features, labels=labels, weights=weights, vectors=vectors, head_weight=head_weight)


loss_scale = 32.0
tiny_eps = 1e-06

def silu_slope(pre_act):
    gate_val = jax.nn.sigmoid(pre_act)
    return gate_val * (1.0 + pre_act * (1.0 - gate_val))

def reference(features, labels, weights, vectors, head_weight):
    micro_count, batch_rows, full_width = features.shape
    layer_count = weights.shape[0]
    hidden = features.reshape(micro_count * batch_rows, full_width)
    sign_all = (2 * labels - 1).astype(jnp.float32).reshape(-1)
    sigmas = []
    new_list = []
    inputs = []
    pre_acts = []
    for layer_index in range(layer_count):
        weight = weights[layer_index]
        vector_bf = vectors[layer_index].astype(jnp.bfloat16)
        left_sum = jnp.dot(weight, vector_bf, preferred_element_type=jnp.float32)
        vector_v = (left_sum * lax.rsqrt(jnp.sum(left_sum * left_sum) + tiny_eps)).astype(jnp.bfloat16)
        right_part = jnp.dot(vector_v, weight, preferred_element_type=jnp.float32)
        spectral = jnp.sqrt(jnp.sum(right_part * right_part) + tiny_eps)
        sigmas.append(spectral)
        new_list.append(right_part / spectral)
        pre_act = jnp.dot(hidden, weight, preferred_element_type=jnp.float32) / spectral
        inputs.append(hidden)
        pre_acts.append(pre_act)
        hidden = (hidden.astype(jnp.float32) + jax.nn.silu(pre_act)).astype(jnp.bfloat16)
    logit_row = lax.optimization_barrier(jnp.sum(hidden.astype(jnp.float32) * head_weight[None, :], axis=1))
    top_scale = -loss_scale * sign_all * jax.nn.sigmoid(-sign_all * logit_row)
    grad_hidden = (top_scale[:, None] * head_weight[None, :]).astype(jnp.bfloat16)
    grad_list = [None] * layer_count
    coef_list = [None] * layer_count
    for layer_index in reversed(range(layer_count)):
        weight = weights[layer_index]
        spectral = sigmas[layer_index]
        grad_pre = (grad_hidden.astype(jnp.float32) * silu_slope(pre_acts[layer_index])).astype(jnp.bfloat16)
        outer_sum = jnp.dot(inputs[layer_index].T, grad_pre, preferred_element_type=jnp.float32)
        grad_list[layer_index] = (outer_sum / spectral).astype(jnp.bfloat16)
        coef_list[layer_index] = jnp.sum(outer_sum * weight.astype(jnp.float32)) / (spectral * spectral)
        if layer_index > 0:
            back_sum = jnp.dot(grad_pre, weight.T, preferred_element_type=jnp.float32)
            grad_hidden = (grad_hidden.astype(jnp.float32) + back_sum / spectral).astype(jnp.bfloat16)
    return (jnp.stack(grad_list), jnp.stack(new_list), jnp.stack(coef_list))
```

```python
import jax
import jax.numpy as jnp
from jax import lax
from jax.experimental import pallas as pl
from jax.experimental.pallas import tpu as pltpu
from jax.sharding import PartitionSpec as P


loss_scale = 32.0
tiny_eps = 1e-06
extra_rows = 8


def silu_slope(pre_act):
    gate_val = jax.nn.sigmoid(pre_act)
    return gate_val * (1.0 + pre_act * (1.0 - gate_val))


def stages_of(size):
    bits = [1 << b for b in reversed(range(size.bit_length() - 1))]
    assert size == 1 << len(bits)
    head = [tuple(bits[:2])] if bits[:2] else []
    return head + [(b,) for b in bits[2:]]


def masks_of(bits):
    masks = [0]
    for b in reversed(bits):
        masks += [m | b for m in masks]
    return masks


def swap(block, mask):
    size = lax.axis_size("mp")
    return lax.ppermute(block, "mp", [(i, i ^ mask) for i in range(size)])


def hop(block, distance):
    size = lax.axis_size("section")
    return lax.ppermute(block, "section", [(i, (i + distance) % size) for i in range(size)])


def split(total):
    high = lax.reduce_precision(total, 8, 7)
    rest = total - high
    mid = lax.reduce_precision(rest, 8, 7)
    return high.astype(jnp.bfloat16), mid.astype(jnp.bfloat16), (rest - mid).astype(jnp.bfloat16)


def sum_all(part):
    for bits in reversed(stages_of(lax.axis_size("mp"))):
        for b in reversed(bits):
            part = part + swap(part, b)
    return part


def gather(block):
    size, place = lax.axis_size("mp"), lax.axis_index("mp")
    rows, width = block.shape
    have = {0: block}
    for bits in stages_of(size):
        new = {}
        if len(have) == 1:
            for m in masks_of(bits)[1:]:
                new[m] = swap(block, m)
        else:
            keys = list(have)
            for half in (keys[: len(keys) // 2], keys[len(keys) // 2 :]) if bits[0] > 1 else (keys,):
                got = swap(jnp.concatenate([have[k] for k in half], axis=1), bits[0])
                for spot, k in enumerate(half):
                    new[k | bits[0]] = got[:, spot * width : (spot + 1) * width]
        have |= new
    whole = jnp.zeros((rows, size * width), block.dtype)
    for k, piece in have.items():
        whole = lax.dynamic_update_slice(whole, piece, (0, (place ^ k) * width))
    return whole


def scatter_sum(total, extra, width):
    size, place = lax.axis_size("mp"), lax.axis_index("mp")
    rows = total.shape[0]

    def pack(extra):
        lanes = jnp.concatenate(split(extra))
        lanes = jnp.pad(lanes, (0, extra_rows * width - lanes.size))
        return lanes.reshape(extra_rows, width)

    def unpack(tail):
        lanes = tail.astype(jnp.float32).reshape(-1)
        return lanes[:rows] + lanes[rows : 2 * rows] + lanes[2 * rows : 3 * rows]

    stages = stages_of(size)
    count = size
    for (bit,) in reversed(stages[1:]):
        mine = (place // bit) % 2 == 1
        even = [total[:, i * width : (i + 1) * width] for i in range(0, count, 2)]
        odd = [total[:, i * width : (i + 1) * width] for i in range(1, count, 2)]
        send = [jnp.where(mine, e, o).astype(jnp.bfloat16) for e, o in zip(even, odd, strict=True)]
        keep = [jnp.where(mine, o, e) for e, o in zip(even, odd, strict=True)]
        count //= 2
        body = jnp.concatenate(send, axis=1)
        tail = pack(extra)
        if count > 1:
            tail = jnp.concatenate([tail, jnp.zeros((extra_rows, (count - 1) * width), jnp.bfloat16)], axis=1)
        got = swap(jnp.concatenate([body, tail], axis=0), bit)
        total = jnp.concatenate(keep, axis=1) + got[:rows].astype(jnp.float32)
        extra = extra + unpack(got[rows:, :width])
    top = place // (size // count)
    result = lax.dynamic_slice_in_dim(total, top * width, width, 1)
    tail, extra_in = pack(extra), extra
    for m in reversed(masks_of(stages[0])[1:]):
        spot = (place ^ m) // (size // count)
        body = lax.dynamic_slice_in_dim(total, spot * width, width, 1).astype(jnp.bfloat16)
        got = swap(jnp.concatenate([body, tail], axis=0), m)
        result = result + got[:rows].astype(jnp.float32)
        extra = extra + unpack(got[rows:])
    return result, extra


def many_sections(features, labels, weights, vectors, head_weight):
    weight = weights[0]
    micro_count, batch_rows, width = features.shape
    rows = micro_count * batch_rows
    sections = lax.axis_size("section")
    section = lax.axis_index("section")
    size, place = lax.axis_size("mp"), lax.axis_index("mp")
    sign_all = (2 * labels - 1).astype(jnp.float32).reshape(rows)
    last = section == sections - 1

    hidden = gather(features.reshape(rows, width))

    vector_bf = vectors[0].astype(jnp.bfloat16)
    left_sum = sum_all(jnp.dot(weight, vector_bf, preferred_element_type=jnp.float32))
    vector_v = (left_sum * lax.rsqrt(jnp.sum(left_sum * left_sum) + tiny_eps)).astype(jnp.bfloat16)
    right_part = jnp.dot(vector_v, weight, preferred_element_type=jnp.float32)
    norm_part = split(jnp.sum(right_part * right_part))
    norm_rows = jnp.stack([jnp.full((width,), n) for n in norm_part])

    product = jnp.dot(hidden, weight, preferred_element_type=jnp.float32)
    sent = hop(jnp.concatenate([product.astype(jnp.bfloat16), norm_rows]), 1)
    zeros = jnp.zeros((2, width), jnp.bfloat16)
    whole = gather(jnp.concatenate([sent, norm_rows, zeros]))
    norms = jnp.sum(whole[rows:].astype(jnp.float32), axis=1) / width
    before = jnp.sqrt(norms[0] + norms[1] + norms[2] + tiny_eps)
    spectral = jnp.sqrt(norms[3] + norms[4] + norms[5] + tiny_eps)
    step = jax.nn.silu(whole[:rows].astype(jnp.float32) / before)
    hidden = (hidden.astype(jnp.float32) + jnp.where(section >= 1, step, 0.0)).astype(jnp.bfloat16)
    for layer in range(1, sections):
        product = jnp.dot(hidden, weight, preferred_element_type=jnp.float32)
        pre_act = product / spectral
        mine = lax.dynamic_slice_in_dim(hidden, place * width, width, 1)
        out = (mine.astype(jnp.float32) + jax.nn.silu(pre_act)).astype(jnp.bfloat16)
        if layer < sections - 1:
            whole = gather(hop(out, 1))
            hidden = jnp.where(section > layer, whole, hidden)
    partial_logit = jnp.sum(out.astype(jnp.float32) * head_weight[None, :], axis=1)

    slope = silu_slope(pre_act)
    head_rows = jnp.broadcast_to(head_weight[None, :], (rows, width))
    grad_out = head_rows
    for layer in range(sections - 1, 0, -1):
        grad_pre = (grad_out * slope).astype(jnp.bfloat16)
        partial_term = lax.dot_general(
            grad_pre, weight, (((1,), (1,)), ((), ())), preferred_element_type=jnp.float32
        )
        back_sum, logit = scatter_sum(partial_term, partial_logit, width)
        grad_in = grad_out + back_sum / spectral
        if layer == sections - 1:
            top_scale = -loss_scale * sign_all * jax.nn.sigmoid(-sign_all * logit)
            grad_in = grad_in * top_scale[:, None]
            grad_out = jnp.where(last, top_scale[:, None] * head_rows, grad_out)
        came = hop(grad_in.astype(jnp.bfloat16), -1).astype(jnp.float32)
        grad_out = jnp.where(section == layer - 1, came, grad_out)
    grad_pre = (grad_out * slope).astype(jnp.bfloat16)
    outer_sum = lax.dot_general(
        hidden, grad_pre, (((0,), (0,)), ((), ())), preferred_element_type=jnp.float32
    )
    weight_grad = (outer_sum / spectral).astype(jnp.bfloat16)
    inner_total = sum_all(jnp.sum(grad_pre.astype(jnp.float32) * product).reshape(1, 1))
    rank_coef = inner_total / (spectral * spectral)
    return (weight_grad[None], (right_part / spectral)[None], rank_coef.reshape(1))


def fast_memory(count):
    return [pl.BlockSpec(memory_space=pltpu.VMEM) for _ in range(count)]


def call(body, outs, args, flops, scratch=(), first_spec=None):
    specs = fast_memory(len(args))
    if first_spec is not None:
        specs[0] = first_spec
    return pl.pallas_call(
        body,
        in_specs=specs,
        out_specs=fast_memory(len(outs)),
        out_shape=[jax.ShapeDtypeStruct(shape, kind) for shape, kind in outs],
        scratch_shapes=list(scratch),
        cost_estimate=pl.CostEstimate(flops=flops, transcendentals=0, bytes_accessed=0),
        compiler_params=pltpu.CompilerParams(vmem_limit_bytes=40 << 20),
    )(*args)


f32, bf16 = jnp.float32, jnp.bfloat16


def matmul(left, right):
    return jnp.dot(left, right, preferred_element_type=f32)


def matmul_t(left, right):
    return lax.dot_general(left, right, (((1,), (1,)), ((), ())), preferred_element_type=f32)


def in_three(total):
    high = total.astype(bf16).astype(f32)
    rest = total - high
    mid = rest.astype(bf16).astype(f32)
    return high, mid, rest - mid


def load_weight(weight, vector_u):
    full, width = weight.shape
    size = full // width

    def body(hbm, vec, kept, product, sems):
        copies = [
            pltpu.make_async_copy(hbm.at[pl.ds(i * width, width)], kept.at[pl.ds(i * width, width)], sems.at[i])
            for i in range(size)
        ]
        for c in copies:
            c.start()
        left = jnp.broadcast_to(vec[...], (16, width)).astype(bf16)
        for i, c in enumerate(copies):
            c.wait()
            rows = matmul_t(left, kept[i * width : (i + 1) * width, :])
            product[i : i + 1, :] = rows[:1]

    return call(
        body,
        [((full, width), bf16), ((size, width), f32)],
        (weight, vector_u),
        2 * full * width * 16,
        [pltpu.SemaphoreType.DMA((size,))],
        pl.BlockSpec(memory_space=pl.ANY),
    )


def spots(pieces, width):
    found = {}
    for i, (keys, _) in enumerate(pieces):
        for j, k in enumerate(keys):
            found[k] = (i, slice(j * width, (j + 1) * width))
    return found


def relay_gather(block):
    size = lax.axis_size("mp")
    near, far = stages_of(size)[1:], stages_of(size)[0]
    have = [((0,), block)]
    for m in masks_of(far)[1:]:
        have.append(((m,), swap(block, m)))
    for (bit,) in near:
        if bit > 1:
            pairs = [have[i : i + 2] for i in range(0, len(have), 2)]
        else:
            pairs = [have]
        new = []
        for group in pairs:
            keys = tuple(k for ks, _ in group for k in ks)
            new.append((tuple(k | bit for k in keys), swap(jnp.concatenate([b for _, b in group], axis=1), bit)))
        have = have + new
    return have


def first_product(weight, pieces, sums, place, width):
    size = weight.shape[0] // width
    rows = pieces[0][1].shape[0]
    where = spots(pieces, width)
    blocks = [b for _, b in pieces]

    def body(*refs):
        index, kept, left_a, left_b = refs[:4]
        ins = refs[4 : 4 + len(blocks)]
        message, right, norms, vec = refs[4 + len(blocks) :]
        me = index[0]
        left_sum = left_a[...] + left_b[...]
        vec[...] = left_sum * lax.rsqrt(jnp.sum(left_sum * left_sum, keepdims=True) + tiny_eps)
        total = jnp.zeros((rows + 16, width), f32)
        for k in range(size):
            i, cols = where[k]
            row = jnp.broadcast_to(vec[pl.ds(me ^ k, 1), :], (16, width)).astype(bf16)
            left = jnp.concatenate([ins[i][:, cols], row], axis=0)
            total = total + matmul(left, kept[pl.ds(pl.multiple_of((me ^ k) * width, width), width), :])
        message[:rows, :] = total[:rows].astype(bf16)
        part = total[rows : rows + 1]
        right[...] = part
        high, mid, low = in_three(jnp.sum(part * part, keepdims=True))
        line = lax.broadcasted_iota(jnp.int32, (extra_rows, width), 0)
        own = jnp.where(line % 3 == 0, high, jnp.where(line % 3 == 1, mid, low))
        own = jnp.where(line < 6, own, 0.0)
        message[rows:, :] = own.astype(bf16)
        norms[...] = own.astype(bf16)

    return call(
        body,
        [((rows + extra_rows, width), bf16), ((1, width), f32), ((extra_rows, width), bf16)],
        (place, weight, *sums, *blocks),
        2 * size * width * width * rows,
        [pltpu.VMEM((size, width), f32)],
        pl.BlockSpec(memory_space=pltpu.SMEM),
    )


def second_layer(weight, pieces, came, head, right_part, place, is_last, width):
    size = weight.shape[0] // width
    rows = pieces[0][1].shape[0]
    where, where_came = spots(pieces, width), spots(came, width)
    blocks, blocks_came = [b for _, b in pieces], [b for _, b in came]
    half = size // 2

    def body(*refs):
        index, kept, head_in, right = refs[:4]
        ins = refs[4 : 4 + len(blocks)]
        ins_came = refs[4 + len(blocks) : 4 + len(blocks) + len(blocks_came)]
        (send, keep, extra, hidden, slope_out, grad_out, roots, new_vec, ratio) = refs[4 + len(blocks) + len(blocks_came) :]
        me, live = index[0], index[1]
        norms = jnp.zeros((extra_rows, width), f32)
        for k in range(size):
            i, cols = where_came[k]
            norms = norms + ins_came[i][rows:, cols].astype(f32)
        before = jnp.sqrt(norms[0:1] + norms[1:2] + norms[2:3] + tiny_eps)
        own = jnp.sqrt(norms[3:4] + norms[4:5] + norms[5:6] + tiny_eps)
        roots[0:1, :] = before
        roots[1:2, :] = own
        new_vec[...] = right[...] / own
        back = 1.0 / before
        mask = jnp.where(live == 1, 1.0, 0.0)
        total = jnp.zeros((rows, width), f32)
        for k in range(size):
            i, cols = where[k]
            ic, cols_c = where_came[k]
            act = ins_came[ic][:rows, cols_c].astype(f32)
            pre = act * back
            gate = jax.nn.sigmoid(pre)
            ratio[k] = act * (gate * (1.0 + pre * (1.0 - gate)))
            now = (ins[i][:, cols].astype(f32) + mask * (pre * gate)).astype(bf16)
            hidden[k] = now
            total = total + matmul(now, kept[pl.ds(pl.multiple_of((me ^ k) * width, width), width), :])
        pre = total / own
        gate = jax.nn.sigmoid(pre)
        slope = gate * (1.0 + pre * (1.0 - gate))
        out = (hidden[0].astype(f32) + pre * gate).astype(bf16).astype(f32)
        head_row = head_in[...]
        slope_out[...] = slope
        grad = head_row * slope
        grad_out[...] = grad
        grad_bf = grad.astype(bf16)
        logit = jnp.sum(out * head_row, axis=1, keepdims=True)
        inner = jnp.sum(grad * total, axis=1, keepdims=True)
        cross = head_row * ratio[0]
        over = 1.0 / own
        for k in range(size):
            part = matmul_t(grad_bf, kept[pl.ds(pl.multiple_of((me ^ k) * width, width), width), :])
            cross = cross + part * (ratio[k] * over)
            cols = slice((k // 2) * width, (k // 2 + 1) * width)
            if k % 2:
                send[:rows, cols] = part.astype(bf16)
            else:
                keep[:, cols] = part
        cross = jnp.sum(cross, axis=1, keepdims=True)
        lane = lax.broadcasted_iota(jnp.int32, (rows, rows), 1)
        table = jnp.where(lane == 0, logit, jnp.where(lane == 1, inner, jnp.where(lane == 2, cross, 0.0)))
        table = table.T[:extra_rows]
        extra[...] = table
        send[rows:, :] = jnp.zeros((extra_rows, half * width), bf16)
        put_extra(send, table, rows)

    wide = (rows + extra_rows, half * width)
    return call(
        body,
        [
            (wide, bf16),
            ((rows, half * width), f32),
            ((extra_rows, rows), f32),
            ((size, rows, width), bf16),
            ((rows, width), f32),
            ((rows, width), f32),
            ((2, width), f32),
            ((1, width), f32),
        ],
        (place, weight, head, right_part, *blocks, *blocks_came),
        4 * size * width * width * rows,
        [pltpu.VMEM((size, rows, width), f32)],
        pl.BlockSpec(memory_space=pltpu.SMEM),
    )


def put_extra(ref, table, rows):
    for spot, part in enumerate(in_three(table)):
        ref[rows:, spot * rows : (spot + 1) * rows] = part.astype(bf16)


def get_extra(ref, rows):
    return sum(ref[rows:, spot * rows : (spot + 1) * rows].astype(f32) for spot in range(3))


def add_near(keep, got, extra, width):
    rows = keep.shape[0]
    count = keep.shape[1] // width
    order = [range(count // 2 + 1, count, 2), range(1, count // 2, 2)]

    def body(kept, came, extra_in, first, second, stay, extra_out):
        table = extra_in[...] + get_extra(came, rows)
        extra_out[...] = table
        for ref, spots_out in zip((first, second), order, strict=True):
            ref[rows:, :] = jnp.zeros((extra_rows, ref.shape[1]), bf16)
            for j, s in enumerate(spots_out):
                cols = slice(s * width, (s + 1) * width)
                ref[:rows, j * width : (j + 1) * width] = (kept[:, cols] + came[:rows, cols].astype(f32)).astype(bf16)
        put_extra(first, table, rows)
        for j, s in enumerate(range(0, count, 2)):
            cols = slice(s * width, (s + 1) * width)
            stay[:, j * width : (j + 1) * width] = kept[:, cols] + came[:rows, cols].astype(f32)

    quarter = (rows + extra_rows, count // 4 * width)
    return call(
        body,
        [(quarter, bf16), (quarter, bf16), ((rows, count // 2 * width), f32), ((extra_rows, rows), f32)],
        (keep, got, extra),
        rows * count * width,
    )


def add_far(stay, got, extra, width):
    rows = stay.shape[0]

    def body(kept, came, extra_in, one, two, extra_out):
        table = extra_in[...] + get_extra(came, rows)
        extra_out[...] = table
        for j, ref in enumerate((one, two)):
            cols = slice(j * width, (j + 1) * width)
            mine = slice((2 + j) * width, (3 + j) * width)
            ref[:rows, :] = (kept[:, mine] + came[:rows, cols].astype(f32)).astype(bf16)
            ref[rows:, :] = jnp.zeros((extra_rows, width), bf16)
            put_extra(ref, table, rows)

    message = (rows + extra_rows, width)
    return call(body, [(message, bf16), (message, bf16), ((extra_rows, rows), f32)], (stay, got, extra), rows * width)


def add_last(stay, got, extra, width):
    rows = stay.shape[0]

    def body(kept, came, extra_in, one, own):
        one[:rows, :] = (kept[:, width : 2 * width] + came[:rows, width:].astype(f32)).astype(bf16)
        one[rows:, :] = jnp.zeros((extra_rows, width), bf16)
        put_extra(one, extra_in[...], rows)
        own[...] = kept[:, :width] + came[:rows, :width].astype(f32)

    return call(body, [((rows + extra_rows, width), bf16), ((rows, width), f32)], (stay, got, extra), rows * width)


def close_sum(own, got, extra, head, grad, roots, sign_row, width):
    rows = own.shape[0]

    def body(mine, a, b, c, extra_in, head_in, grad_in, roots_in, sign_in, message, grad_out, coef):
        table = extra_in[...] + get_extra(a, rows) + get_extra(b, rows) + get_extra(c, rows)
        sign = sign_in[...]
        scale = -loss_scale * sign * jax.nn.sigmoid(-sign * table[0:1])
        before, last = roots_in[0:1, :1], roots_in[1:2, :1]
        coef[...] = jnp.broadcast_to(jnp.sum(scale * table[1:2], axis=1, keepdims=True) / (last * last), coef.shape)
        lower = jnp.sum(scale * table[2:3], axis=1, keepdims=True) / (before * before)
        tall = jnp.broadcast_to(scale, (rows, rows)).T[:, :1]
        total = mine[...] + a[:rows, :].astype(f32) + b[:rows, :].astype(f32) + c[:rows, :].astype(f32)
        message[:rows, :] = (tall * (head_in[...] + total / last)).astype(bf16)
        grad_out[...] = (tall * grad_in[...]).astype(bf16)
        line = lax.broadcasted_iota(jnp.int32, (extra_rows, width), 0)
        high, mid, low = in_three(lower)
        parts = jnp.where(line == 0, high, jnp.where(line == 1, mid, jnp.where(line == 2, low, 0.0)))
        message[rows:, :] = parts.astype(bf16)

    return call(
        body,
        [((rows + extra_rows, width), bf16), ((rows, width), bf16), ((1, 128), f32)],
        (own, *got, extra, head, grad, roots, sign_row),
        rows * width,
    )


def weight_gradient(hidden, came, slope, grad, roots, coef, place, width):
    size, rows, _ = hidden.shape

    def body(index, acts, message, slope_in, own, roots_in, coef_in, out, coef_out, factor):
        k = pl.program_id(0)
        last = index[1] == 1

        @pl.when(k == 0)
        def _():
            lower = (message[:rows, :].astype(f32) * slope_in[...]).astype(bf16)
            factor[...] = jnp.where(last, own[...], lower)
            parts = message[rows:, :128].astype(f32)
            coef_out[...] = jnp.where(last, coef_in[...], parts[0:1] + parts[1:2] + parts[2:3])

        total = lax.dot_general(acts[k], factor[...], (((0,), (0,)), ((), ())), preferred_element_type=f32)
        out[...] = (total * (1.0 / roots_in[1:2, :])).astype(bf16)

    whole = pl.BlockSpec(memory_space=pltpu.VMEM)
    return pl.pallas_call(
        body,
        grid_spec=pltpu.PrefetchScalarGridSpec(
            num_scalar_prefetch=1,
            grid=(size,),
            in_specs=[whole] * 6,
            out_specs=[pl.BlockSpec((width, width), lambda k, index: (index[0] ^ k, 0)), whole],
            scratch_shapes=[pltpu.VMEM((rows, width), bf16)],
        ),
        out_shape=[jax.ShapeDtypeStruct((size * width, width), bf16), jax.ShapeDtypeStruct((1, 128), f32)],
        cost_estimate=pl.CostEstimate(flops=2 * size * rows * width * width, transcendentals=0, bytes_accessed=0),
        compiler_params=pltpu.CompilerParams(vmem_limit_bytes=40 << 20),
    )(place, hidden, came, slope, grad, roots, coef)


def two_sections(features, labels, weights, vectors, head_weight):
    micro_count, batch_rows, width = features.shape
    rows = micro_count * batch_rows
    position, section = lax.axis_index("mp"), lax.axis_index("section")
    place = jnp.stack([position, section]).astype(jnp.int32)
    sign_row = (2 * labels - 1).astype(f32).reshape(1, rows)
    head = head_weight.reshape(1, width)

    pieces = relay_gather(features.reshape(rows, width))
    weight, part = load_weight(weights[0], vectors)
    for bits in reversed(stages_of(lax.axis_size("mp"))):
        for b in reversed(bits):
            sums = (part, swap(part, b))
            part = sums[0] + sums[1]
    message, right_part, norms = first_product(weight, pieces, sums, place, width)
    line = lax.broadcasted_iota(jnp.int32, message.shape, 0)
    own = jnp.pad(norms, ((rows, 0), (0, 0)))
    came = relay_gather(jnp.where((line >= rows + 3) & (line < rows + 6), own, hop(message, 1)))
    send, keep, extra, hidden, slope, grad, roots, new_vector = second_layer(
        weight, pieces, came, head, right_part, place, section, width
    )
    first, second, stay, extra = add_near(keep, swap(send, 1), extra, width)
    got_first, got_second = swap(first, 2), swap(second, 2)
    two, three, extra = add_far(stay, got_first, extra, width)
    far = masks_of(stages_of(lax.axis_size("mp"))[0])
    got_two, got_three = swap(two, far[2]), swap(three, far[3])
    one, own_sum = add_last(stay, got_second, extra, width)
    got_one = swap(one, far[1])
    message, grad, coef = close_sum(own_sum, (got_one, got_two, got_three), extra, head, grad, roots, sign_row, width)
    weight_grad, rank_coef = weight_gradient(hidden, hop(message, -1), slope, grad, roots, coef, place, width)
    return (weight_grad[None], new_vector, rank_coef[0, :1])


def on_device(*args):
    if lax.axis_size("section") == 2 and len(stages_of(lax.axis_size("mp"))) == 3:
        return two_sections(*args)
    return many_sections(*args)


def solution(mesh):
    placed = (P(None, None, "mp"), P(), P("section", None, "mp"), P("section", "mp"), P("mp"))
    return jax.shard_map(
        on_device,
        mesh=mesh,
        in_specs=placed,
        out_specs=(P("section", None, "mp"), P("section", "mp"), P("section")),
        check_vma=False,
    )
```

```python
import jax
import jax.numpy as jnp
from jax import lax
from jax.experimental import pallas as pl
from jax.experimental.pallas import tpu as pltpu
from jax.sharding import PartitionSpec as P


loss_scale = 32.0
tiny_eps = 1e-06
extra_rows = 8


def silu_slope(pre_act):
    gate_val = jax.nn.sigmoid(pre_act)
    return gate_val * (1.0 + pre_act * (1.0 - gate_val))


def stages_of(size):
    bits = [1 << b for b in reversed(range(size.bit_length() - 1))]
    assert size == 1 << len(bits)
    head = [tuple(bits[:2])] if bits[:2] else []
    return head + [(b,) for b in bits[2:]]


def masks_of(bits):
    masks = [0]
    for b in reversed(bits):
        masks += [m | b for m in masks]
    return masks


def swap(block, mask):
    size = lax.axis_size("mp")
    return lax.ppermute(block, "mp", [(i, i ^ mask) for i in range(size)])


def hop(block, distance):
    size = lax.axis_size("section")
    return lax.ppermute(block, "section", [(i, (i + distance) % size) for i in range(size)])


def send_down(block, mask):
    size, count = lax.axis_size("mp"), lax.axis_size("section")
    pairs = [(i, (i - size) ^ mask if i >= size else i + (count - 1) * size) for i in range(count * size)]
    return lax.ppermute(block, ("section", "mp"), pairs)


def split(total):
    high = lax.reduce_precision(total, 8, 7)
    rest = total - high
    mid = lax.reduce_precision(rest, 8, 7)
    return high.astype(jnp.bfloat16), mid.astype(jnp.bfloat16), (rest - mid).astype(jnp.bfloat16)


def sum_all(part):
    for bits in reversed(stages_of(lax.axis_size("mp"))):
        for b in reversed(bits):
            part = part + swap(part, b)
    return part


def gather(block):
    size, place = lax.axis_size("mp"), lax.axis_index("mp")
    rows, width = block.shape
    have = {0: block}
    for bits in stages_of(size):
        new = {}
        if len(have) == 1:
            for m in masks_of(bits)[1:]:
                new[m] = swap(block, m)
        else:
            keys = list(have)
            for half in (keys[: len(keys) // 2], keys[len(keys) // 2 :]) if bits[0] > 1 else (keys,):
                got = swap(jnp.concatenate([have[k] for k in half], axis=1), bits[0])
                for spot, k in enumerate(half):
                    new[k | bits[0]] = got[:, spot * width : (spot + 1) * width]
        have |= new
    whole = jnp.zeros((rows, size * width), block.dtype)
    for k, piece in have.items():
        whole = lax.dynamic_update_slice(whole, piece, (0, (place ^ k) * width))
    return whole


def scatter_sum(total, extra, width):
    size, place = lax.axis_size("mp"), lax.axis_index("mp")
    rows = total.shape[0]

    def pack(extra):
        lanes = jnp.concatenate(split(extra))
        lanes = jnp.pad(lanes, (0, extra_rows * width - lanes.size))
        return lanes.reshape(extra_rows, width)

    def unpack(tail):
        lanes = tail.astype(jnp.float32).reshape(-1)
        return lanes[:rows] + lanes[rows : 2 * rows] + lanes[2 * rows : 3 * rows]

    stages = stages_of(size)
    count = size
    for (bit,) in reversed(stages[1:]):
        mine = (place // bit) % 2 == 1
        even = [total[:, i * width : (i + 1) * width] for i in range(0, count, 2)]
        odd = [total[:, i * width : (i + 1) * width] for i in range(1, count, 2)]
        send = [jnp.where(mine, e, o).astype(jnp.bfloat16) for e, o in zip(even, odd, strict=True)]
        keep = [jnp.where(mine, o, e) for e, o in zip(even, odd, strict=True)]
        count //= 2
        body = jnp.concatenate(send, axis=1)
        tail = pack(extra)
        if count > 1:
            tail = jnp.concatenate([tail, jnp.zeros((extra_rows, (count - 1) * width), jnp.bfloat16)], axis=1)
        got = swap(jnp.concatenate([body, tail], axis=0), bit)
        total = jnp.concatenate(keep, axis=1) + got[:rows].astype(jnp.float32)
        extra = extra + unpack(got[rows:, :width])
    top = place // (size // count)
    result = lax.dynamic_slice_in_dim(total, top * width, width, 1)
    tail = pack(extra)
    for m in reversed(masks_of(stages[0])[1:]):
        spot = (place ^ m) // (size // count)
        body = lax.dynamic_slice_in_dim(total, spot * width, width, 1).astype(jnp.bfloat16)
        got = swap(jnp.concatenate([body, tail], axis=0), m)
        result = result + got[:rows].astype(jnp.float32)
        extra = extra + unpack(got[rows:])
    return result, extra


def many_sections(features, labels, weights, vectors, head_weight):
    weight = weights[0]
    micro_count, batch_rows, width = features.shape
    rows = micro_count * batch_rows
    sections = lax.axis_size("section")
    section = lax.axis_index("section")
    place = lax.axis_index("mp")
    sign_all = (2 * labels - 1).astype(jnp.float32).reshape(rows)
    last = section == sections - 1

    hidden = gather(features.reshape(rows, width))

    vector_bf = vectors[0].astype(jnp.bfloat16)
    left_sum = sum_all(jnp.dot(weight, vector_bf, preferred_element_type=jnp.float32))
    vector_v = (left_sum * lax.rsqrt(jnp.sum(left_sum * left_sum) + tiny_eps)).astype(jnp.bfloat16)
    right_part = jnp.dot(vector_v, weight, preferred_element_type=jnp.float32)
    norm_part = split(jnp.sum(right_part * right_part))
    norm_rows = jnp.stack([jnp.full((width,), n) for n in norm_part])

    product = jnp.dot(hidden, weight, preferred_element_type=jnp.float32)
    sent = hop(jnp.concatenate([product.astype(jnp.bfloat16), norm_rows]), 1)
    zeros = jnp.zeros((2, width), jnp.bfloat16)
    whole = gather(jnp.concatenate([sent, norm_rows, zeros]))
    norms = jnp.sum(whole[rows:].astype(jnp.float32), axis=1) / width
    before = jnp.sqrt(norms[0] + norms[1] + norms[2] + tiny_eps)
    spectral = jnp.sqrt(norms[3] + norms[4] + norms[5] + tiny_eps)
    step = jax.nn.silu(whole[:rows].astype(jnp.float32) / before)
    hidden = (hidden.astype(jnp.float32) + jnp.where(section >= 1, step, 0.0)).astype(jnp.bfloat16)
    for layer in range(1, sections):
        product = jnp.dot(hidden, weight, preferred_element_type=jnp.float32)
        pre_act = product / spectral
        mine = lax.dynamic_slice_in_dim(hidden, place * width, width, 1)
        out = (mine.astype(jnp.float32) + jax.nn.silu(pre_act)).astype(jnp.bfloat16)
        if layer < sections - 1:
            whole = gather(hop(out, 1))
            hidden = jnp.where(section > layer, whole, hidden)
    partial_logit = jnp.sum(out.astype(jnp.float32) * head_weight[None, :], axis=1)

    slope = silu_slope(pre_act)
    head_rows = jnp.broadcast_to(head_weight[None, :], (rows, width))
    grad_out = head_rows
    for layer in range(sections - 1, 0, -1):
        grad_pre = (grad_out * slope).astype(jnp.bfloat16)
        partial_term = lax.dot_general(
            grad_pre, weight, (((1,), (1,)), ((), ())), preferred_element_type=jnp.float32
        )
        back_sum, logit = scatter_sum(partial_term, partial_logit, width)
        grad_in = grad_out + back_sum / spectral
        if layer == sections - 1:
            top_scale = -loss_scale * sign_all * jax.nn.sigmoid(-sign_all * logit)
            grad_in = grad_in * top_scale[:, None]
            grad_out = jnp.where(last, top_scale[:, None] * head_rows, grad_out)
        came = hop(grad_in.astype(jnp.bfloat16), -1).astype(jnp.float32)
        grad_out = jnp.where(section == layer - 1, came, grad_out)
    grad_pre = (grad_out * slope).astype(jnp.bfloat16)
    outer_sum = lax.dot_general(
        hidden, grad_pre, (((0,), (0,)), ((), ())), preferred_element_type=jnp.float32
    )
    weight_grad = (outer_sum / spectral).astype(jnp.bfloat16)
    inner_total = sum_all(jnp.sum(grad_pre.astype(jnp.float32) * product).reshape(1, 1))
    rank_coef = inner_total / (spectral * spectral)
    return (weight_grad[None], (right_part / spectral)[None], rank_coef.reshape(1))


def fast_memory(count):
    return [pl.BlockSpec(memory_space=pltpu.VMEM) for _ in range(count)]


def call(body, outs, args, flops, scratch=(), first_spec=None, limit=4):
    specs = fast_memory(len(args))
    if first_spec is not None:
        specs[0] = first_spec
    return pl.pallas_call(
        body,
        in_specs=specs,
        out_specs=fast_memory(len(outs)),
        out_shape=[jax.ShapeDtypeStruct(shape, kind) for shape, kind in outs],
        scratch_shapes=list(scratch),
        cost_estimate=pl.CostEstimate(flops=flops, transcendentals=0, bytes_accessed=0),
        compiler_params=pltpu.CompilerParams(vmem_limit_bytes=limit << 20),
    )(*args)


f32, bf16 = jnp.float32, jnp.bfloat16


def matmul(left, right):
    return jnp.dot(left, right, preferred_element_type=f32)


def matmul_t(left, right):
    return lax.dot_general(left, right, (((1,), (1,)), ((), ())), preferred_element_type=f32)


def in_three(total):
    high = total.astype(bf16).astype(f32)
    rest = total - high
    mid = rest.astype(bf16).astype(f32)
    return high, mid, rest - mid


def stage(vector_u):
    def body(vec, out):
        out[...] = jnp.broadcast_to(vec[...], out.shape).astype(bf16)

    return call(body, [((16, vector_u.shape[1]), bf16)], (vector_u,), 1 << 34)[0]


def left_product(weight, vector_u):
    full, width = weight.shape
    size = full // width

    def body(kept, vec, product):
        left = vec[...]
        for i in range(size):
            product[i : i + 1, :] = matmul_t(left, kept[i * width : (i + 1) * width, :])[:1]

    return call(body, [((size, width), f32)], (weight, vector_u), 2 * full * width * 16)[0]


def spots(pieces, rows):
    found = {}
    for i, (keys, _) in enumerate(pieces):
        for j, k in enumerate(keys):
            found[k] = (i, j * rows)
    return found


def pack(blocks):
    rows, width = blocks[0].shape

    def body(*refs):
        for i, ref in enumerate(refs[:-1]):
            refs[-1][i * rows : (i + 1) * rows, :] = ref[...]

    return call(body, [((len(blocks) * rows, width), blocks[0].dtype)], blocks, len(blocks) * rows * width)[0]


def add(left, right):
    def body(one, two, out):
        out[...] = one[...] + two[...]

    return call(body, [(left.shape, left.dtype)], (left, right), left.size)[0]


def relay_gather(block):
    size = lax.axis_size("mp")
    near, far = stages_of(size)[1:], stages_of(size)[0]
    have = [((0,), block)]
    for m in masks_of(far)[1:]:
        have.append(((m,), swap(block, m)))
    for stage, (bit,) in enumerate(near):
        groups = [((k,), b) for (k,), b in have[2:]] if stage == 0 else have
        if stage == 0:
            groups = [(have[0][0] + have[1][0], pack([b for _, b in have[:2]]))] + groups
        new = []
        for keys, b in groups:
            new.append((tuple(k | bit for k in keys), swap(b, bit)))
        have = groups + new
    return have


def first_product(weight, pieces, sums, width):
    size = weight.shape[0] // width
    rows = pieces[0][1].shape[0] // len(pieces[0][0])
    where = spots(pieces, rows)
    blocks = [b for _, b in pieces]

    def body(*refs):
        kept, left_a, left_b = refs[:3]
        ins = refs[3 : 3 + len(blocks)]
        message, right, norms, vec = refs[3 + len(blocks) :]
        me = lax.axis_index("mp")
        left_sum = left_a[...] + left_b[...]
        vec[...] = left_sum * lax.rsqrt(jnp.sum(left_sum * left_sum, keepdims=True) + tiny_eps)
        total = jnp.zeros((rows + 16, width), f32)
        for k in range(size):
            i, top = where[k]
            row = jnp.broadcast_to(vec[pl.ds(me ^ k, 1), :], (16, width)).astype(bf16)
            left = jnp.concatenate([ins[i][top : top + rows, :], row], axis=0)
            total = total + matmul(left, kept[pl.ds(pl.multiple_of((me ^ k) * width, width), width), :])
        message[:rows, :] = total[:rows].astype(bf16)
        part = total[rows : rows + 1]
        right[...] = part
        norm = jnp.sum(part * part, keepdims=True)
        high, mid, low = in_three(norm)
        line = lax.broadcasted_iota(jnp.int32, (extra_rows, width), 0)
        own = jnp.where(line == 0, high, jnp.where(line == 1, mid, jnp.where(line == 2, low, 0.0)))
        message[rows:, :] = own.astype(bf16)
        norms[...] = jnp.broadcast_to(norm, norms.shape)

    return call(
        body,
        [((rows + extra_rows, width), bf16), ((1, width), f32), ((8, 128), f32)],
        (weight, *sums, *blocks),
        2 * size * width * width * rows,
        [pltpu.VMEM((size, width), f32)],
    )


def second_layer(weight, pieces, came, norm, head, right_part, width):
    size = weight.shape[0] // width
    rows = pieces[0][1].shape[0] // len(pieces[0][0])
    where, where_came = spots(pieces, rows), spots(came, rows + extra_rows)
    blocks, blocks_came = [b for _, b in pieces], [b for _, b in came]
    half = size // 2

    def body(*refs):
        kept, norm_in, head_in, right = refs[:4]
        refs = refs[1:]
        ins = refs[3 : 3 + len(blocks)]
        ins_came = refs[3 + len(blocks) : 3 + len(blocks) + len(blocks_came)]
        (send, keep, extra, hidden, slope_out, grad_out, roots, new_vec, ratio) = refs[3 + len(blocks) + len(blocks_came) :]
        me, live = lax.axis_index("mp"), lax.axis_index("section")
        norms = jnp.zeros((extra_rows, width), f32)
        for k in range(size):
            i, top = where_came[k]
            norms = norms + ins_came[i][top + rows : top + rows + extra_rows, :].astype(f32)
        before = jnp.sqrt(norms[0:1] + norms[1:2] + norms[2:3] + tiny_eps)
        own = jnp.sqrt(jnp.broadcast_to(norm_in[0:1, :1], (1, width)) + tiny_eps)
        roots[0:1, :] = before
        roots[1:2, :] = own
        new_vec[...] = right[...] / own
        back = 1.0 / before
        mask = jnp.where(live == 1, 1.0, 0.0)
        total = jnp.zeros((rows, width), f32)
        for k in range(size):
            i, top = where[k]
            ic, top_c = where_came[k]
            act = ins_came[ic][top_c : top_c + rows, :].astype(f32)
            pre = act * back
            gate = jax.nn.sigmoid(pre)
            ratio[k] = act * (gate * (1.0 + pre * (1.0 - gate)))
            now = (ins[i][top : top + rows, :].astype(f32) + mask * (pre * gate)).astype(bf16)
            hidden[me ^ k] = now
            mine = now if k == 0 else mine
            total = total + matmul(now, kept[pl.ds(pl.multiple_of((me ^ k) * width, width), width), :])
        pre = total / own
        gate = jax.nn.sigmoid(pre)
        slope = gate * (1.0 + pre * (1.0 - gate))
        out = (mine.astype(f32) + pre * gate).astype(bf16).astype(f32)
        head_row = head_in[...]
        slope_out[...] = slope
        grad = head_row * slope
        grad_out[...] = grad
        grad_bf = grad.astype(bf16)
        logit = jnp.sum(out * head_row, axis=1, keepdims=True)
        inner = jnp.sum(grad * total, axis=1, keepdims=True)
        cross = head_row * ratio[0]
        over = 1.0 / own
        for k in range(size):
            part = matmul_t(grad_bf, kept[pl.ds(pl.multiple_of((me ^ k) * width, width), width), :])
            cross = cross + part * (ratio[k] * over)
            cols = slice((k // 2) * width, (k // 2 + 1) * width)
            if k % 2:
                send[:rows, cols] = part.astype(bf16)
            else:
                keep[:, cols] = part
        cross = jnp.sum(cross, axis=1, keepdims=True)
        lane = lax.broadcasted_iota(jnp.int32, (rows, rows), 1)
        table = jnp.where(lane == 0, logit, jnp.where(lane == 1, inner, jnp.where(lane == 2, cross, 0.0)))
        table = table.T[:extra_rows]
        extra[...] = table
        send[rows:, :] = jnp.zeros((extra_rows, half * width), bf16)
        put_extra(send, table, rows)

    wide = (rows + extra_rows, half * width)
    return call(
        body,
        [
            (wide, bf16),
            ((rows, half * width), f32),
            ((extra_rows, rows), f32),
            ((size, rows, width), bf16),
            ((rows, width), f32),
            ((rows, width), f32),
            ((2, width), f32),
            ((1, width), f32),
        ],
        (weight, norm, head, right_part, *blocks, *blocks_came),
        4 * size * width * width * rows,
        [pltpu.VMEM((size, rows, width), f32)],
        limit=12,
    )


def put_extra(ref, table, rows):
    for spot, part in enumerate(in_three(table)):
        ref[rows:, spot * rows : (spot + 1) * rows] = part.astype(bf16)


def get_extra(ref, rows):
    return sum(ref[rows:, spot * rows : (spot + 1) * rows].astype(f32) for spot in range(3))


def add_near(keep, got, extra, width):
    rows = keep.shape[0]
    count = keep.shape[1] // width
    order, rest = range(count - 1, 0, -2), range(0, count, 2)

    def body(kept, came, extra_in, *outs):
        table = extra_in[...] + get_extra(came, rows)
        stay, extra_out = outs[len(order) :]
        extra_out[...] = table

        def total(s):
            cols = slice(s * width, (s + 1) * width)
            return kept[:, cols] + came[:rows, cols].astype(f32)

        for ref, s in zip(outs, order, strict=False):
            ref[:rows, :] = total(s).astype(bf16)
        outs[0][rows:, :] = jnp.zeros((extra_rows, width), bf16)
        put_extra(outs[0], table, rows)
        for j, s in enumerate(rest):
            stay[:, j * width : (j + 1) * width] = total(s)

    full, bare = ((rows + extra_rows, width), bf16), ((rows, width), bf16)
    outs = [full] + [bare] * (len(order) - 1) + [((rows, len(rest) * width), f32), ((extra_rows, rows), f32)]
    return call(body, outs, (keep, got, extra), rows * count * width)


def add_far(stay, spot, got, extra, width):
    rows = stay.shape[0]
    carries = got.shape[0] > rows

    def body(kept, came, extra_in, out, extra_out):
        table = extra_in[...]
        if carries:
            table = table + get_extra(came, rows)
        extra_out[...] = table
        out[:rows, :] = (kept[:, spot * width : (spot + 1) * width] + came[:rows, :].astype(f32)).astype(bf16)
        out[rows:, :] = jnp.zeros((extra_rows, width), bf16)
        put_extra(out, table, rows)

    outs = [((rows + extra_rows, width), bf16), ((extra_rows, rows), f32)]
    return call(body, outs, (stay, got, extra), rows * width)


def cross(block, mask):
    size, count = lax.axis_size("mp"), lax.axis_size("section")
    pairs = [(i, (i // size + 1) % count * size + (i % size ^ mask)) for i in range(count * size)]
    return lax.ppermute(block, ("section", "mp"), pairs)


def relay_next(message, norms):
    near, far = stages_of(lax.axis_size("mp"))[1:], masks_of(stages_of(lax.axis_size("mp"))[0])
    bit = near[0][0]
    have = []
    for m in far:
        have.append(((m,), cross(message, m)))
    for b in (1, bit, far[1], far[2]):
        norms = add(norms, swap(norms, b))
    have = [((0, far[1]), pack([b for _, b in have[:2]]))] + have[2:]
    for b in (bit, 1):
        new = []
        for keys, piece in have:
            new.append((tuple(k | b for k in keys), swap(piece, b)))
        have = have + new
    return have, norms


def as_row(table):
    count, width = table.shape
    size = count * width
    lane = lax.broadcasted_iota(jnp.int32, (width, size), 1)
    spread = (lane % width == lax.broadcasted_iota(jnp.int32, (width, size), 0)).astype(bf16)
    wide = matmul(table.astype(bf16), spread)
    mine = lax.broadcasted_iota(jnp.int32, (count, size), 1) // width == lax.broadcasted_iota(jnp.int32, (count, size), 0)
    return jnp.sum(jnp.where(mine, wide, 0.0), axis=0, keepdims=True)


def turn(hidden):
    size, rows, width = hidden.shape

    def body(acts, out):
        for i in range(size):
            out[i] = acts[i].T

    return call(body, [((size, width, rows), bf16)], (hidden,), size * rows * width)[0]


def weight_gradient(turned, came, table, slope, grad, roots, head, labels, width):
    size, _, rows = turned.shape

    def body(acts, *refs):
        parts, refs = refs[: len(came)], refs[len(came) :]
        table_in, slope_in, own, roots_in, head_in, sign_in, out, coef, blocks, sems = refs
        last = lax.axis_index("section") == 1
        sums = sum(get_extra(part, rows) for part in parts)
        sums = jnp.where(last, table_in[...], sums)
        sign = as_row((2 * sign_in[...] - 1).astype(f32))
        scale = -loss_scale * sign * jax.nn.sigmoid(-sign * sums[0:1])
        other, over = 1.0 / roots_in[0:1, :], 1.0 / roots_in[1:2, :]
        inner = jnp.sum(scale * jnp.where(last, sums[1:2], sums[2:3]), axis=1, keepdims=True)
        coef[...] = inner * (over * over)[:, :128]
        tall = jnp.broadcast_to(scale, (rows, rows)).T[:, :1]
        total = sum(part[:rows, :].astype(f32) for part in parts)
        lower = (head_in[...] + total * other) * slope_in[...]
        factor = (tall * jnp.where(last, own[...], lower) * over).astype(bf16)
        copies = [
            pltpu.make_async_copy(blocks.at[i], out.at[pl.ds(i * width, width)], sems.at[i]) for i in range(size)
        ]
        for i, copy in enumerate(copies):
            blocks[i] = matmul(acts[i], factor).astype(bf16)
            copy.start()
        for copy in copies:
            copy.wait()

    whole = pl.BlockSpec(memory_space=pltpu.VMEM)
    return pl.pallas_call(
        body,
        in_specs=[whole] * (7 + len(came)),
        out_specs=[pl.BlockSpec(memory_space=pl.ANY), whole],
        scratch_shapes=[pltpu.VMEM((size, width, width), bf16), pltpu.SemaphoreType.DMA((size,))],
        out_shape=[jax.ShapeDtypeStruct((size * width, width), bf16), jax.ShapeDtypeStruct((1, 128), f32)],
        cost_estimate=pl.CostEstimate(flops=2 * size * rows * width * width, transcendentals=0, bytes_accessed=0),
        compiler_params=pltpu.CompilerParams(vmem_limit_bytes=14 << 20),
        name="outer",
    )(turned, *came, table, slope, grad, roots, head, labels)


def two_sections(features, labels, weights, vectors, head_weight):
    micro_count, batch_rows, width = features.shape
    rows = micro_count * batch_rows
    head = head_weight.reshape(1, width)

    weight = weights[0]
    pieces = relay_gather(features.reshape(rows, width))
    part = left_product(weight, stage(vectors))
    for bits in reversed(stages_of(lax.axis_size("mp"))):
        for b in reversed(bits):
            sums = (part, swap(part, b))
            part = add(*sums)
    message, right_part, norms = first_product(weight, pieces, sums, width)
    came, norm = relay_next(message, norms)
    send, keep, extra, hidden, slope, grad, roots, new_vector = second_layer(
        weight, pieces, came, norm, head, right_part, width
    )
    got = swap(send, 1)
    far = masks_of(stages_of(lax.axis_size("mp"))[0])
    bit = stages_of(lax.axis_size("mp"))[1][0]
    *parts, stay, table = add_near(keep, got, extra, width)
    for spot in reversed(range(len(far))):
        parts[-1 - spot] = swap(parts[-1 - spot], bit)
    came = []
    for spot in reversed(range(len(far))):
        part, table = add_far(stay, spot, parts[-1 - spot], table, width)
        came.append(send_down(part, far[spot]))
        if spot == len(far) - 1:
            total = table
    for b in far[1:3]:
        total = add(total, swap(total, b))
    turned = turn(hidden)
    weight_grad, rank_coef = weight_gradient(turned, came, total, slope, grad, roots, head, labels, width)
    return (weight_grad[None], new_vector, rank_coef[0, :1])


def on_device(*args):
    if lax.axis_size("section") == 2 and len(stages_of(lax.axis_size("mp"))) == 3:
        return two_sections(*args)
    return many_sections(*args)


def solution(mesh):
    placed = (P(None, None, "mp"), P(), P("section", None, "mp"), P("section", "mp"), P("mp"))
    return jax.shard_map(
        on_device,
        mesh=mesh,
        in_specs=placed,
        out_specs=(P("section", None, "mp"), P("section", "mp"), P("section")),
        check_vma=False,
    )
```
